32 devices in a mesh: px: 4 (over y, x), py: 8 (over z, core).
Axes of the slice: x: 2, y: 2, z: 4, core: 2. Of those that a mesh axis runs over, the one named last changes fastest.
Arguments:
- white_noise: float32 [2, 64, 256, 256], P(None, 'px', 'py'), may hold values from -6 to 6
- spectrum: float32 [64, 256, 256], P('px', 'py'), may hold values from 0.1 to 2, as said below
- group_table: int32 [3, 8], replicated, may hold values from 0 to 7, each once within a row
Outputs:
- modulus: float32 [2, 64, 256, 256], P(None, 'px', 'py')
- level_one: float32 [2, 32, 128, 128], P(None, 'px', 'py')
- level_two: float32 [2, 16, 64, 64], P(None, 'px', 'py')
- level_three: float32 [2, 8, 32, 32], P(None, 'px', 'py')
The draws below stay inside these ranges and needn't reach their ends.
Inputs may be any that keep to these rules, and one draw needn't show every extreme that they name: spectrum[j, m, k] equals spectrum[(64 - j) % 64, (256 - m) % 256, (256 - k) % 256]. `group_table`: each row is a permutation of 0 to 7.
All inputs are finite; a program needn't handle non-finite values.
Results may differ from the reference program's by a relative error of at most 0.000088.
Values sent between devices are 32-bit elements; how exact they have to be, the bound alone decides.
A program may use at most 192 MiB of HBM per device.

```python
import math
import jax
import jax.numpy as jnp

FIELDS = 2
LEVELS = 3
NZ = 256
NX = 64
NY = 256
N_PY = 8


def draw_spectrum(key, part):
    log_low = math.log(0.1)
    log_high = math.log(2.0)
    rough_part = jnp.exp(jax.random.uniform(key, (NX, NY, NZ), jnp.float32, log_low, log_high))
    mirror = jnp.roll(jnp.flip(rough_part, (0, 1, 2)), 1, (0, 1, 2))
    values = 0.5 * (rough_part + mirror)
    return values


def level_of(stream_key, extent, shards, low, top_value):
    def one(axis_at, blocks):
        draws = jax.random.uniform(jax.random.fold_in(jax.random.fold_in(stream_key, 6), axis_at), (blocks,), jnp.float32, low / len(shards), top_value / len(shards))
        return jnp.repeat(jnp.exp(draws), extent[axis_at] // blocks).reshape((-1,) + (1,) * (len(extent) - axis_at - 1))

    level = one(*shards[0])
    for cut in shards[1:]:
        level = level * one(*cut)
    return level


def normal_values(own_key, shape, deviation, most, split=(), dtype=jnp.bfloat16):
    array = jax.random.normal(own_key, shape, jnp.float32) * deviation
    if len(split) > 0:
        array = level_of(own_key, shape, split, -0.22, 0.18) * array
    return jnp.clip(array, min=-most, max=most).astype(dtype)


def setup_inputs(seed: int = 0) -> dict:
    arg_keys = jax.random.split(jax.random.key(seed), 4)
    white_noise = normal_values(arg_keys[0], (FIELDS, NX, NY, NZ), 1.0, 6.0, ((1, 4), (2, 8)), jnp.float32)
    spectrum = draw_spectrum(jax.random.fold_in(arg_keys[3], 71), 0)
    group_table = jax.vmap(lambda own: jax.random.permutation(own, N_PY))(jax.random.split(arg_keys[2], LEVELS)).reshape((LEVELS, N_PY)).astype(jnp.int32)
    return dict(white_noise=white_noise, spectrum=spectrum, group_table=group_table)


def coarsen(values):
    members, size_x, size_y, size_z = values.shape
    blocks = values.reshape(members, size_x // 2, 2, size_y // 2, 2, size_z // 2, 2)
    return blocks.mean(axis=(2, 4, 6))


def route_blocks(coarse, group_order):
    members, size_x, size_y, size_z = coarse.shape
    blocks = coarse.reshape(members, size_x, N_PY, size_y // N_PY, size_z)
    picked = jnp.take(blocks, group_order, axis=2)
    return picked.reshape(members, size_x, size_y, size_z)


def reference(white_noise, spectrum, group_table):
    spectra = jnp.fft.fftn(white_noise, axes=(1, 2, 3))
    scaled = spectra * spectrum[None]
    fields_real = jnp.real(jnp.fft.ifftn(scaled, axes=(1, 2, 3)))
    modulus = jnp.exp(0.5 * fields_real)
    coarse_one = coarsen(modulus)
    coarse_two = coarsen(coarse_one)
    coarse_three = coarsen(coarse_two)
    level_one = route_blocks(coarse_one, group_table[0])
    level_two = route_blocks(coarse_two, group_table[1])
    level_three = route_blocks(coarse_three, group_table[2])
    return modulus, level_one, level_two, level_three
```

```python
import numpy as np

import jax
import jax.numpy as jnp
from jax import lax
from jax.sharding import PartitionSpec as P


def angles_of(length):
    positions = np.arange(length, dtype=np.int64)
    return (positions[:, None] * positions[None, :] % length) * (2.0 * np.pi / length)


def complex_table(length, direction):
    angles = angles_of(length)
    cos, sin = np.cos(angles), direction * np.sin(angles)
    table = np.stack([np.stack([cos, sin], 1), np.stack([-sin, cos], 1)], 0)
    return jnp.asarray(table, jnp.float32)


def half_tables(length):
    angles = angles_of(length)[:, : length // 2]
    ahead = np.stack([np.cos(angles), -np.sin(angles)], 1)
    back = 2.0 * ahead
    nyquist = np.where(np.arange(length) % 2 == 0, 1.0, -1.0)
    ahead[:, 1, 0] = nyquist
    back[:, 0, 0] = 1.0
    back[:, 1, 0] = nyquist
    return jnp.asarray(ahead, jnp.float32), jnp.asarray(back, jnp.float32)


def einsum(pattern, left, right):
    return jnp.einsum(pattern, left, right, precision=lax.Precision.HIGH)


def swap_first(values):
    first = values[:, :, :1]
    turned = jnp.swapaxes(first, 0, 1)
    return jnp.concatenate([turned, values[:, :, 1:]], 2)


def coarsen(values):
    members, size_x, size_y, size_z = values.shape
    blocks = values.reshape(members, size_x // 2, 2, size_y // 2, 2, size_z // 2, 2)
    return blocks.mean(axis=(2, 4, 6))


def on_device(white_noise, spectrum, group_table):
    members, cells_x, cells_y, length_z = white_noise.shape
    size_px, size_py = lax.axis_size("px"), lax.axis_size("py")
    length_x, length_y = cells_x * size_px, cells_y * size_py
    half_z = length_z // 2
    block_py, block = half_z // size_py, half_z // size_py // size_px
    z_ahead, z_back = half_tables(length_z)
    scale = 1.0 / (length_x * length_y * length_z)

    table = jnp.transpose(spectrum, (2, 0, 1))
    last = jnp.broadcast_to(table[half_z : half_z + 1], (size_py, 1, cells_x, cells_y))
    table = jnp.concatenate([table[:half_z].reshape(size_py, block_py, cells_x, cells_y), last], 1)
    table = lax.all_to_all(table, "py", split_axis=0, concat_axis=3, tiled=True)[0]
    last = jnp.broadcast_to(table[block_py:], (size_px, 1, cells_x, length_y))
    table = jnp.concatenate([table[:block_py].reshape(size_px, block, cells_x, length_y), last], 1)
    table = lax.all_to_all(table, "px", split_axis=0, concat_axis=2, tiled=True)[0] * scale
    is_first = (lax.axis_index("px") == 0) & (lax.axis_index("py") == 0)
    other = jnp.where(is_first, table[block:], table[:1])
    tables = jnp.stack([table[:block], jnp.concatenate([other, table[1:block]], 0)], 0)

    values = einsum("fxyz,zck->fckxy", white_noise, z_ahead)
    values = swap_first(values)
    values = lax.all_to_all(values, "py", split_axis=2, concat_axis=4, tiled=True)
    values = einsum("fckxy,cydm->fdkxm", values, complex_table(length_y, -1.0))
    values = lax.all_to_all(values, "px", split_axis=2, concat_axis=3, tiled=True)
    values = einsum("fckxm,cxdj->fdkjm", values, complex_table(length_x, -1.0))
    values = values * tables[:, None]
    values = einsum("fckjm,cjdx->fdkxm", values, complex_table(length_x, 1.0))
    values = lax.all_to_all(values, "px", split_axis=3, concat_axis=2, tiled=True)
    values = einsum("fckxm,cmdy->fdkxy", values, complex_table(length_y, 1.0))
    values = lax.all_to_all(values, "py", split_axis=4, concat_axis=2, tiled=True)
    values = swap_first(values)
    fields = einsum("fckxy,zck->fxyz", values, z_back)
    modulus = jnp.exp(0.5 * fields)

    levels = []
    level = modulus
    for _ in range(3):
        level = coarsen(level)
        levels.append(level)
    pieces = [jnp.reshape(level, (size_py, -1)) for level in levels]
    widths = [piece.shape[1] for piece in pieces]
    joined = jnp.concatenate(pieces, 1)
    spread = lax.all_to_all(joined, "py", split_axis=0, concat_axis=0, tiled=True)
    picked, start = [], 0
    for index, width in enumerate(widths):
        part = spread[:, start : start + width]
        picked.append(jnp.take(part, group_table[index], axis=0))
        start += width
    joined = lax.all_to_all(
        jnp.concatenate(picked, 1), "py", split_axis=0, concat_axis=0, tiled=True
    )
    routed, start = [], 0
    for level, width in zip(levels, widths):
        routed.append(joined[:, start : start + width].reshape(level.shape))
        start += width
    return (modulus, routed[0], routed[1], routed[2])


def solution(mesh):
    in_specs = (P(None, "px", "py", None), P("px", "py", None), P())
    out_specs = (P(None, "px", "py", None),) * 4
    return jax.shard_map(
        on_device, mesh=mesh, in_specs=in_specs, out_specs=out_specs, check_vma=False
    )
```

```python
import numpy as np

import jax
import jax.numpy as jnp
from jax import lax
from jax.experimental import pallas as pl
from jax.experimental.pallas import tpu as pltpu
from jax.sharding import PartitionSpec as P


def angles_of(length):
    positions = np.arange(length, dtype=np.int64)
    return (positions[:, None] * positions[None, :] % length) * (2.0 * np.pi / length)


def complex_array(length, direction):
    angles = angles_of(length)
    cos, sin = np.cos(angles), direction * np.sin(angles)
    return np.stack([np.stack([cos, sin], 1), np.stack([-sin, cos], 1)], 0)


def complex_table(length, direction):
    return jnp.asarray(complex_array(length, direction), jnp.float32)


def half_tables(length):
    angles = angles_of(length)[:, : length // 2]
    ahead = np.stack([np.cos(angles), -np.sin(angles)], 1)
    back = 2.0 * ahead
    nyquist = np.where(np.arange(length) % 2 == 0, 1.0, -1.0)
    ahead[:, 1, 0] = nyquist
    back[:, 0, 0] = 1.0
    back[:, 1, 0] = nyquist
    return jnp.asarray(ahead, jnp.float32), jnp.asarray(back, jnp.float32)


def einsum(pattern, left, right):
    return jnp.einsum(pattern, left, right, precision=lax.Precision.HIGH)


def swap_first(values):
    first = values[:, :, :1]
    turned = jnp.swapaxes(first, 0, 1)
    return jnp.concatenate([turned, values[:, :, 1:]], 2)


def coarsen(values):
    members, size_x, size_y, size_z = values.shape
    blocks = values.reshape(members, size_x // 2, 2, size_y // 2, 2, size_z // 2, 2)
    return blocks.mean(axis=(2, 4, 6))


def general_path(white_noise, spectrum, group_table):
    members, cells_x, cells_y, length_z = white_noise.shape
    size_px, size_py = lax.axis_size("px"), lax.axis_size("py")
    length_x, length_y = cells_x * size_px, cells_y * size_py
    half_z = length_z // 2
    block_py, block = half_z // size_py, half_z // size_py // size_px
    z_ahead, z_back = half_tables(length_z)
    scale = 1.0 / (length_x * length_y * length_z)

    table = jnp.transpose(spectrum, (2, 0, 1))
    last = jnp.broadcast_to(table[half_z : half_z + 1], (size_py, 1, cells_x, cells_y))
    table = jnp.concatenate([table[:half_z].reshape(size_py, block_py, cells_x, cells_y), last], 1)
    table = lax.all_to_all(table, "py", split_axis=0, concat_axis=3, tiled=True)[0]
    last = jnp.broadcast_to(table[block_py:], (size_px, 1, cells_x, length_y))
    table = jnp.concatenate([table[:block_py].reshape(size_px, block, cells_x, length_y), last], 1)
    table = lax.all_to_all(table, "px", split_axis=0, concat_axis=2, tiled=True)[0] * scale
    is_first = (lax.axis_index("px") == 0) & (lax.axis_index("py") == 0)
    other = jnp.where(is_first, table[block:], table[:1])
    tables = jnp.stack([table[:block], jnp.concatenate([other, table[1:block]], 0)], 0)

    values = einsum("fxyz,zck->fckxy", white_noise, z_ahead)
    values = swap_first(values)
    values = lax.all_to_all(values, "py", split_axis=2, concat_axis=4, tiled=True)
    values = einsum("fckxy,cydm->fdkxm", values, complex_table(length_y, -1.0))
    values = lax.all_to_all(values, "px", split_axis=2, concat_axis=3, tiled=True)
    values = einsum("fckxm,cxdj->fdkjm", values, complex_table(length_x, -1.0))
    values = values * tables[:, None]
    values = einsum("fckjm,cjdx->fdkxm", values, complex_table(length_x, 1.0))
    values = lax.all_to_all(values, "px", split_axis=3, concat_axis=2, tiled=True)
    values = einsum("fckxm,cmdy->fdkxy", values, complex_table(length_y, 1.0))
    values = lax.all_to_all(values, "py", split_axis=4, concat_axis=2, tiled=True)
    values = swap_first(values)
    fields = einsum("fckxy,zck->fxyz", values, z_back)
    modulus = jnp.exp(0.5 * fields)

    levels = []
    level = modulus
    for _ in range(3):
        level = coarsen(level)
        levels.append(level)
    pieces = [jnp.reshape(level, (size_py, -1)) for level in levels]
    widths = [piece.shape[1] for piece in pieces]
    joined = jnp.concatenate(pieces, 1)
    spread = lax.all_to_all(joined, "py", split_axis=0, concat_axis=0, tiled=True)
    picked, start = [], 0
    for index, width in enumerate(widths):
        part = spread[:, start : start + width]
        picked.append(jnp.take(part, group_table[index], axis=0))
        start += width
    joined = lax.all_to_all(
        jnp.concatenate(picked, 1), "py", split_axis=0, concat_axis=0, tiled=True
    )
    routed, start = [], 0
    for level, width in zip(levels, widths):
        routed.append(joined[:, start : start + width].reshape(level.shape))
        start += width
    return (modulus, routed[0], routed[1], routed[2])


LANES = 128


def dot(left, right):
    return jnp.dot(
        left, right, precision=lax.Precision.HIGHEST, preferred_element_type=jnp.float32
    )


def lane_of(shape):
    return lax.broadcasted_iota(jnp.int32, shape, len(shape) - 1)


def exchange(arrays, width):
    arrays = list(arrays)
    lane = lane_of(arrays[0].shape)
    distance = 1
    while distance < len(arrays):
        step = distance * width
        low = (lane // step) % 2 == 0
        for index in range(len(arrays)):
            if (index // distance) % 2 == 0:
                first, second = arrays[index], arrays[index + distance]
                arrays[index] = jnp.where(low, first, pltpu.roll(second, step, 1))
                arrays[index + distance] = jnp.where(
                    low, pltpu.roll(first, LANES - step, 1), second
                )
        distance *= 2
    return arrays


def swap_slot(first, second):
    at_zero = lane_of(first.shape) == 0
    return jnp.where(at_zero, second, first), jnp.where(at_zero, first, second)


def z_forward_kernel(sizes, noise_ref, spectrum_ref, table_ref, out_ref, held):
    lo, hi, kept = sizes
    cells_y = noise_ref.shape[2]
    for f in range(2):
        rows = noise_ref[f].reshape(lo * hi * cells_y, noise_ref.shape[3])
        held[f] = dot(rows, table_ref[...])

    def tile(f, c, x):
        return held[f, pl.ds(x * cells_y, cells_y), pl.ds(c * LANES, LANES)]

    for xh in range(hi):
        tiles = {}
        for xl in range(lo):
            x = xh * lo + xl
            mixed = swap_slot(tile(0, 1, x), tile(1, 0, x))
            members = ((tile(0, 0, x), mixed[0]), (mixed[1], tile(1, 1, x)))
            for f in range(2):
                for c in range(2):
                    tiles[f, c, xl] = members[f][c]
        for f in range(2):
            for c in range(2):
                moved = exchange([tiles[f, c, xl] for xl in range(lo)], kept)
                for p in range(lo):
                    out_ref[p, (f * 2 + c) * hi + xh] = moved[p]
    group = lane_of((cells_y, LANES))
    last = jnp.zeros((cells_y, LANES), jnp.float32)
    for xh in range(hi):
        names = [xh * lo + xl for xl in range(lo)]
        moved = exchange([spectrum_ref[x, :, pl.ds(0, LANES)] for x in names], kept)
        for p in range(lo):
            out_ref[p, 4 * hi + xh] = moved[p]
        for xl in range(lo):
            value = spectrum_ref[names[xl], :, pl.ds(LANES, 1)]
            last = jnp.where(group == xl * kept + xh, value, last)
    for p in range(lo):
        out_ref[p, 5 * hi] = last


def y_forward_kernel(sizes, in_ref, table_ref, out_ref):
    lo, hi, kept = sizes
    length_y = table_ref.shape[1]
    ranks = 2 * hi
    half = length_y // 2

    def whole(t):
        return in_ref[:, t].reshape(length_y, LANES)

    for f in range(2):
        arrays = [None] * ranks
        for xh in range(hi):
            pair = [whole((f * 2 + c) * hi + xh) for c in range(2)]
            product = dot(table_ref[...], jnp.concatenate(pair, 1))
            by_cos, by_sin = product[:length_y], product[length_y:]
            arrays[xh] = by_cos[:, :LANES] + by_sin[:, LANES:]
            arrays[hi + xh] = by_cos[:, LANES:] - by_sin[:, :LANES]
        moved = exchange(arrays, kept // ranks)
        for r in range(ranks):
            out_ref[r, pl.ds(f * length_y, length_y)] = moved[r]
    halves = []
    for mh in range(2):
        for xh in range(hi):
            halves.append(whole(4 * hi + xh)[mh * half : (mh + 1) * half])
    moved = exchange(halves, kept // ranks)
    last = whole(5 * hi)
    packed = last[:half] + pltpu.roll(last[half:], hi, 1)
    for r in range(ranks):
        out_ref[r, pl.ds(2 * length_y, half)] = moved[r]
        out_ref[r, pl.ds(2 * length_y + half, half)] = packed


def x_kernel(sizes, first_ref, in_ref, ahead_ref, back_ref, out_ref):
    lo, hi, kept = sizes
    ranks = 2 * hi
    length_y = out_ref.shape[1] // 2
    half = length_y // 2
    lane = lane_of((half, LANES))
    low = (lane // (hi * ranks)) % 2 == 0
    parts = [in_ref[r, pl.ds(2 * length_y, half)] for r in range(ranks)]
    tables = []
    for part in exchange(parts, 1):
        upper = jnp.where(low, part, pltpu.roll(part, hi * ranks, 1))
        lower = jnp.where(low, pltpu.roll(part, LANES - hi * ranks, 1), part)
        tables.append(jnp.concatenate([upper, lower], 0))
    last = [in_ref[r, pl.ds(2 * length_y + half, half)] for r in range(ranks)]
    last = jnp.concatenate(last, 1)
    source = lax.broadcasted_iota(jnp.int32, (ranks * LANES, LANES), 0)
    target = lax.broadcasted_iota(jnp.int32, (ranks * LANES, LANES), 1)
    same = (source // LANES == target % ranks) & ((source % LANES) // kept == target // kept)
    level = (target // ranks) % hi
    picked = []
    for mh in range(2):
        chosen = same & (source % kept == mh * hi + level)
        picked.append(dot(last, chosen.astype(jnp.float32)))
    last = jnp.concatenate(picked, 0)
    is_first = lax.broadcasted_iota(jnp.int32, last.shape, 0) * 0 + first_ref[0] == 1
    other = jnp.where(is_first, last, tables[0])
    for f in range(2):
        rows = pl.ds(f * length_y, length_y)
        arrays = exchange([in_ref[r, rows] for r in range(ranks)], 1)
        for q in range(ranks):
            table = other if f == 1 and q == 0 else tables[q]
            arrays[q] = dot(dot(arrays[q], ahead_ref[...]) * table, back_ref[...])
        arrays = exchange(arrays, 1)
        for r in range(ranks):
            out_ref[r, rows] = arrays[r]


def y_back_kernel(sizes, in_ref, table_ref, out_ref):
    lo, hi, kept = sizes
    ranks = 2 * hi
    length_y = table_ref.shape[1]
    cells_y = length_y // lo
    for f in range(2):
        rows = pl.ds(f * length_y, length_y)
        arrays = exchange([in_ref[r, rows] for r in range(ranks)], kept // ranks)
        for xh in range(hi):
            product = dot(table_ref[...], jnp.concatenate([arrays[xh], arrays[hi + xh]], 1))
            by_cos, by_sin = product[:length_y], product[length_y:]
            real = by_cos[:, :LANES] - by_sin[:, LANES:]
            imag = by_cos[:, LANES:] + by_sin[:, :LANES]
            out_ref[:, (f * 2) * hi + xh] = real.reshape(lo, cells_y, LANES)
            out_ref[:, (f * 2 + 1) * hi + xh] = imag.reshape(lo, cells_y, LANES)


def pool_matrix(rows, columns, weight, transposed):
    long_axis = 0 if transposed else 1
    shape = (columns, rows) if transposed else (rows, columns)
    long = lax.broadcasted_iota(jnp.int32, shape, long_axis)
    short = lax.broadcasted_iota(jnp.int32, shape, 1 - long_axis)
    return jnp.where(long // 2 == short, weight, 0.0).astype(jnp.float32)


def pool_rows(cells_x, cells_y):
    shape = (cells_x * cells_y // 4, cells_x * cells_y)
    short = lax.broadcasted_iota(jnp.int32, shape, 0)
    long = lax.broadcasted_iota(jnp.int32, shape, 1)
    same_x = long // (2 * cells_y) == short // (cells_y // 2)
    same_y = (long % cells_y) // 2 == short % (cells_y // 2)
    return jnp.where(same_x & same_y, 0.125, 0.0).astype(jnp.float32)


def z_back_kernel(sizes, in_ref, table_ref, modulus_ref, coarse_ref, held):
    lo, hi, kept = sizes
    cells_y = in_ref.shape[2]
    cells_x = lo * hi
    length_z = table_ref.shape[0]
    for xh in range(hi):
        tiles = {}
        for f in range(2):
            for c in range(2):
                arrays = [in_ref[p, (f * 2 + c) * hi + xh] for p in range(lo)]
                tiles[f, c] = exchange(arrays, kept)
        for xl in range(lo):
            mixed = swap_slot(tiles[0, 1][xl], tiles[1, 0][xl])
            members = ((tiles[0, 0][xl], mixed[0]), (mixed[1], tiles[1, 1][xl]))
            rows = pl.ds((xh * lo + xl) * cells_y, cells_y)
            for f in range(2):
                for c in range(2):
                    held[f, rows, pl.ds(c * LANES, LANES)] = members[f][c]
    coarse_ref[...] = jnp.zeros(coarse_ref.shape, jnp.float32)
    for f in range(2):
        values = jnp.exp(0.5 * dot(held[f], table_ref[...]))
        modulus_ref[f] = values.reshape(cells_x, cells_y, length_z)
        size_x, size_y, size_z = cells_x, cells_y, length_z
        start = 0
        for _ in range(3):
            right = pool_matrix(size_z // 2, size_z, 1.0, True)
            values = dot(pool_rows(size_x, size_y), dot(values, right))
            size_x, size_y, size_z = size_x // 2, size_y // 2, size_z // 2
            height = 2 * size_x * size_y // lo
            for d in range(lo // 2):
                piece = values[d * height : (d + 1) * height]
                place = (f * lo // 2 + d, pl.ds(start, height), pl.ds(0, size_z))
                coarse_ref[place] = piece
            start += height


def pick_kernel(heights, table_ref, in_ref, out_ref):
    for column in range(in_ref.shape[0]):
        start = 0
        for index, height in enumerate(heights):
            rows = pl.ds(start, height)
            out_ref[column, rows] = in_ref[table_ref[index, column], rows]
            start += height


def lanes_path(white_noise, spectrum, group_table):
    members, cells_x, cells_y, length_z = white_noise.shape
    size_px, size_py = lax.axis_size("px"), lax.axis_size("py")
    length_x, length_y = cells_x * size_px, cells_y * size_py
    lo, hi = size_py, cells_x // size_py
    kept = LANES // size_py
    sizes = (lo, hi, kept)
    f32 = jnp.float32
    params = pltpu.CompilerParams(vmem_limit_bytes=48 * 1024 * 1024)

    def call(body, shapes, *operands, scratch=(), scalars=0):
        out = [jax.ShapeDtypeStruct(shape, f32) for shape in shapes]
        specs = [pl.BlockSpec(memory_space=pltpu.SMEM)] * scalars
        specs += [pl.BlockSpec(memory_space=pltpu.VMEM)] * (len(operands) - scalars)
        return pl.pallas_call(
            body,
            out_shape=out,
            in_specs=specs,
            out_specs=[pl.BlockSpec(memory_space=pltpu.VMEM)] * len(out),
            scratch_shapes=list(scratch),
            compiler_params=params,
        )(*operands)

    def spread(values, axis):
        return lax.all_to_all(values, axis, split_axis=0, concat_axis=0, tiled=True)

    z_ahead, z_back = half_tables(length_z)
    z_ahead = z_ahead.reshape(length_z, length_z)
    z_back = z_back.reshape(length_z, length_z).T * (1.0 / (length_x * length_y * length_z))
    angles = angles_of(length_y)
    y_table = jnp.asarray(np.concatenate([np.cos(angles), np.sin(angles)], 0), f32)
    lane = np.arange(LANES)
    part = (lane // (hi * size_px)) % 2
    place = (lane % size_px) * cells_x + (lane // size_px % hi) * lo + lane // kept

    def x_table(direction):
        table = complex_array(length_x, direction)
        rows = table[part, place]
        return jnp.asarray(rows[:, part, place], f32)

    first = (lax.axis_index("px") == 0) & (lax.axis_index("py") == 0)
    first = first.astype(jnp.int32).reshape(1)
    held = pltpu.VMEM((members, cells_x * cells_y, length_z), f32)

    def bind(body):
        def bound(*refs):
            body(sizes, *refs)

        return bound

    tiles = 4 * hi
    (values,) = call(
        bind(z_forward_kernel),
        [(size_py, tiles + hi + 1, cells_y, LANES)],
        white_noise,
        spectrum,
        z_ahead,
        scratch=[held],
    )
    values = spread(values, "py")
    (values,) = call(
        bind(y_forward_kernel), [(size_px, 3 * length_y, LANES)], values, y_table
    )
    values = spread(values, "px")
    (values,) = call(
        bind(x_kernel),
        [(size_px, 2 * length_y, LANES)],
        first,
        values,
        x_table(-1.0),
        x_table(1.0),
        scalars=1,
    )
    values = spread(values, "px")
    (values,) = call(
        bind(y_back_kernel), [(size_py, tiles, cells_y, LANES)], values, y_table
    )
    values = spread(values, "py")
    shapes = []
    heights = []
    size = (cells_x, cells_y, length_z)
    for _ in range(3):
        size = tuple(extent // 2 for extent in size)
        shapes.append((members,) + size)
        heights.append(members * size[0] * size[1] // size_py)
    modulus, coarse = call(
        bind(z_back_kernel),
        [white_noise.shape, (size_py, sum(heights), LANES)],
        values,
        z_back,
        scratch=[held],
    )
    coarse = spread(coarse, "py")

    def pick(*refs):
        pick_kernel(heights, *refs)

    (coarse,) = call(pick, [coarse.shape], group_table, coarse, scalars=1)
    coarse = spread(coarse, "py")
    routed, start = [], 0
    for shape, height in zip(shapes, heights):
        routed.append(coarse[:, start : start + height, : shape[3]].reshape(shape))
        start += height
    return (modulus, routed[0], routed[1], routed[2])


def on_device(white_noise, spectrum, group_table):
    members, cells_x, cells_y, length_z = white_noise.shape
    size_px, size_py = lax.axis_size("px"), lax.axis_size("py")
    fits = members == 2 and length_z == 2 * LANES and 2 * cells_x * size_px == LANES
    fits = fits and cells_x * 2 == size_px * size_py
    fits = fits and size_px * size_px * size_py == LANES
    chosen = lanes_path if fits else general_path
    return chosen(white_noise, spectrum, group_table)


def solution(mesh):
    in_specs = (P(None, "px", "py", None), P("px", "py", None), P())
    out_specs = (P(None, "px", "py", None),) * 4
    return jax.shard_map(
        on_device, mesh=mesh, in_specs=in_specs, out_specs=out_specs, check_vma=False
    )
```

```python
import numpy as np

import jax
import jax.numpy as jnp
from jax import lax
from jax.experimental import pallas as pl
from jax.experimental.pallas import tpu as pltpu
from jax.sharding import PartitionSpec as P


def angles_of(length):
    positions = np.arange(length, dtype=np.int64)
    return (positions[:, None] * positions[None, :] % length) * (2.0 * np.pi / length)


def complex_array(length, direction):
    angles = angles_of(length)
    cos, sin = np.cos(angles), direction * np.sin(angles)
    return np.stack([np.stack([cos, sin], 1), np.stack([-sin, cos], 1)], 0)


def complex_table(length, direction):
    return jnp.asarray(complex_array(length, direction), jnp.float32)


def half_tables(length):
    angles = angles_of(length)[:, : length // 2]
    ahead = np.stack([np.cos(angles), -np.sin(angles)], 1)
    back = 2.0 * ahead
    nyquist = np.where(np.arange(length) % 2 == 0, 1.0, -1.0)
    ahead[:, 1, 0] = nyquist
    back[:, 0, 0] = 1.0
    back[:, 1, 0] = nyquist
    return jnp.asarray(ahead, jnp.float32), jnp.asarray(back, jnp.float32)


def einsum(pattern, left, right):
    return jnp.einsum(pattern, left, right, precision=lax.Precision.HIGH)


def swap_first(values):
    first = values[:, :, :1]
    turned = jnp.swapaxes(first, 0, 1)
    return jnp.concatenate([turned, values[:, :, 1:]], 2)


def coarsen(values):
    members, size_x, size_y, size_z = values.shape
    blocks = values.reshape(members, size_x // 2, 2, size_y // 2, 2, size_z // 2, 2)
    return blocks.mean(axis=(2, 4, 6))


def general_path(white_noise, spectrum, group_table):
    members, cells_x, cells_y, length_z = white_noise.shape
    size_px, size_py = lax.axis_size("px"), lax.axis_size("py")
    length_x, length_y = cells_x * size_px, cells_y * size_py
    half_z = length_z // 2
    block_py, block = half_z // size_py, half_z // size_py // size_px
    z_ahead, z_back = half_tables(length_z)
    scale = 1.0 / (length_x * length_y * length_z)

    table = jnp.transpose(spectrum, (2, 0, 1))
    last = jnp.broadcast_to(table[half_z : half_z + 1], (size_py, 1, cells_x, cells_y))
    table = jnp.concatenate([table[:half_z].reshape(size_py, block_py, cells_x, cells_y), last], 1)
    table = lax.all_to_all(table, "py", split_axis=0, concat_axis=3, tiled=True)[0]
    last = jnp.broadcast_to(table[block_py:], (size_px, 1, cells_x, length_y))
    table = jnp.concatenate([table[:block_py].reshape(size_px, block, cells_x, length_y), last], 1)
    table = lax.all_to_all(table, "px", split_axis=0, concat_axis=2, tiled=True)[0] * scale
    is_first = (lax.axis_index("px") == 0) & (lax.axis_index("py") == 0)
    other = jnp.where(is_first, table[block:], table[:1])
    tables = jnp.stack([table[:block], jnp.concatenate([other, table[1:block]], 0)], 0)

    values = einsum("fxyz,zck->fckxy", white_noise, z_ahead)
    values = swap_first(values)
    values = lax.all_to_all(values, "py", split_axis=2, concat_axis=4, tiled=True)
    values = einsum("fckxy,cydm->fdkxm", values, complex_table(length_y, -1.0))
    values = lax.all_to_all(values, "px", split_axis=2, concat_axis=3, tiled=True)
    values = einsum("fckxm,cxdj->fdkjm", values, complex_table(length_x, -1.0))
    values = values * tables[:, None]
    values = einsum("fckjm,cjdx->fdkxm", values, complex_table(length_x, 1.0))
    values = lax.all_to_all(values, "px", split_axis=3, concat_axis=2, tiled=True)
    values = einsum("fckxm,cmdy->fdkxy", values, complex_table(length_y, 1.0))
    values = lax.all_to_all(values, "py", split_axis=4, concat_axis=2, tiled=True)
    values = swap_first(values)
    fields = einsum("fckxy,zck->fxyz", values, z_back)
    modulus = jnp.exp(0.5 * fields)

    levels = []
    level = modulus
    for _ in range(3):
        level = coarsen(level)
        levels.append(level)
    pieces = [jnp.reshape(level, (size_py, -1)) for level in levels]
    widths = [piece.shape[1] for piece in pieces]
    joined = jnp.concatenate(pieces, 1)
    spread = lax.all_to_all(joined, "py", split_axis=0, concat_axis=0, tiled=True)
    picked, start = [], 0
    for index, width in enumerate(widths):
        part = spread[:, start : start + width]
        picked.append(jnp.take(part, group_table[index], axis=0))
        start += width
    joined = lax.all_to_all(
        jnp.concatenate(picked, 1), "py", split_axis=0, concat_axis=0, tiled=True
    )
    routed, start = [], 0
    for level, width in zip(levels, widths):
        routed.append(joined[:, start : start + width].reshape(level.shape))
        start += width
    return (modulus, routed[0], routed[1], routed[2])


LANES = 128
MESH = pl.DeviceIdType.MESH


def dot(left, right):
    return jnp.dot(
        left, right, precision=lax.Precision.HIGHEST, preferred_element_type=jnp.float32
    )


def lane_of(shape):
    return lax.broadcasted_iota(jnp.int32, shape, len(shape) - 1)


def exchange(arrays, width):
    arrays = list(arrays)
    lane = lane_of(arrays[0].shape)
    distance = 1
    while distance < len(arrays):
        step = distance * width
        low = (lane // step) % 2 == 0
        for index in range(len(arrays)):
            if (index // distance) % 2 == 0:
                first, second = arrays[index], arrays[index + distance]
                arrays[index] = jnp.where(low, first, pltpu.roll(second, step, 1))
                arrays[index + distance] = jnp.where(
                    low, pltpu.roll(first, LANES - step, 1), second
                )
        distance *= 2
    return arrays


def swap_slot(first, second):
    at_zero = lane_of(first.shape) == 0
    return jnp.where(at_zero, second, first), jnp.where(at_zero, first, second)


def z_forward_kernel(sizes, noise_ref, spectrum_ref, table_ref, out_ref, held):
    lo, hi, kept = sizes
    cells_y = noise_ref.shape[2]
    for f in range(2):
        rows = noise_ref[f].reshape(lo * hi * cells_y, noise_ref.shape[3])
        held[f] = dot(rows, table_ref[...])

    def tile(f, c, x):
        return held[f, pl.ds(x * cells_y, cells_y), pl.ds(c * LANES, LANES)]

    for xh in range(hi):
        tiles = {}
        for xl in range(lo):
            x = xh * lo + xl
            mixed = swap_slot(tile(0, 1, x), tile(1, 0, x))
            members = ((tile(0, 0, x), mixed[0]), (mixed[1], tile(1, 1, x)))
            for f in range(2):
                for c in range(2):
                    tiles[f, c, xl] = members[f][c]
        for f in range(2):
            for c in range(2):
                moved = exchange([tiles[f, c, xl] for xl in range(lo)], kept)
                for p in range(lo):
                    out_ref[p, (f * 2 + c) * hi + xh] = moved[p]
    group = lane_of((cells_y, LANES))
    last = jnp.zeros((cells_y, LANES), jnp.float32)
    for xh in range(hi):
        names = [xh * lo + xl for xl in range(lo)]
        moved = exchange([spectrum_ref[x, :, pl.ds(0, LANES)] for x in names], kept)
        for p in range(lo):
            out_ref[p, 4 * hi + xh] = moved[p]
        for xl in range(lo):
            value = spectrum_ref[names[xl], :, pl.ds(LANES, 1)]
            last = jnp.where(group == xl * kept + xh, value, last)
    for p in range(lo):
        out_ref[p, 5 * hi] = last


def y_forward_kernel(sizes, in_ref, table_ref, out_ref):
    lo, hi, kept = sizes
    length_y = table_ref.shape[1]
    ranks = 2 * hi
    half = length_y // 2

    def whole(t):
        return in_ref[:, t].reshape(length_y, LANES)

    for f in range(2):
        arrays = [None] * ranks
        for xh in range(hi):
            pair = [whole((f * 2 + c) * hi + xh) for c in range(2)]
            product = dot(table_ref[...], jnp.concatenate(pair, 1))
            by_cos, by_sin = product[:length_y], product[length_y:]
            arrays[xh] = by_cos[:, :LANES] + by_sin[:, LANES:]
            arrays[hi + xh] = by_cos[:, LANES:] - by_sin[:, :LANES]
        moved = exchange(arrays, kept // ranks)
        for r in range(ranks):
            out_ref[r, pl.ds(f * length_y, length_y)] = moved[r]
    halves = []
    for mh in range(2):
        for xh in range(hi):
            halves.append(whole(4 * hi + xh)[mh * half : (mh + 1) * half])
    moved = exchange(halves, kept // ranks)
    last = whole(5 * hi)
    packed = last[:half] + pltpu.roll(last[half:], hi, 1)
    for r in range(ranks):
        out_ref[r, pl.ds(2 * length_y, half)] = moved[r]
        out_ref[r, pl.ds(2 * length_y + half, half)] = packed


def x_kernel(sizes, first_ref, in_ref, ahead_ref, back_ref, out_ref):
    lo, hi, kept = sizes
    ranks = 2 * hi
    length_y = out_ref.shape[1] // 2
    half = length_y // 2
    lane = lane_of((half, LANES))
    low = (lane // (hi * ranks)) % 2 == 0
    parts = [in_ref[r, pl.ds(2 * length_y, half)] for r in range(ranks)]
    tables = []
    for part in exchange(parts, 1):
        upper = jnp.where(low, part, pltpu.roll(part, hi * ranks, 1))
        lower = jnp.where(low, pltpu.roll(part, LANES - hi * ranks, 1), part)
        tables.append(jnp.concatenate([upper, lower], 0))
    last = [in_ref[r, pl.ds(2 * length_y + half, half)] for r in range(ranks)]
    last = jnp.concatenate(last, 1)
    source = lax.broadcasted_iota(jnp.int32, (ranks * LANES, LANES), 0)
    target = lax.broadcasted_iota(jnp.int32, (ranks * LANES, LANES), 1)
    same = (source // LANES == target % ranks) & ((source % LANES) // kept == target // kept)
    level = (target // ranks) % hi
    picked = []
    for mh in range(2):
        chosen = same & (source % kept == mh * hi + level)
        picked.append(dot(last, chosen.astype(jnp.float32)))
    last = jnp.concatenate(picked, 0)
    is_first = lax.broadcasted_iota(jnp.int32, last.shape, 0) * 0 + first_ref[0] == 1
    other = jnp.where(is_first, last, tables[0])
    for f in range(2):
        rows = pl.ds(f * length_y, length_y)
        arrays = exchange([in_ref[r, rows] for r in range(ranks)], 1)
        for q in range(ranks):
            table = other if f == 1 and q == 0 else tables[q]
            arrays[q] = dot(dot(arrays[q], ahead_ref[...]) * table, back_ref[...])
        arrays = exchange(arrays, 1)
        for r in range(ranks):
            out_ref[r, rows] = arrays[r]


def y_back_kernel(sizes, in_ref, table_ref, out_ref):
    lo, hi, kept = sizes
    ranks = 2 * hi
    length_y = table_ref.shape[1]
    cells_y = length_y // lo
    for f in range(2):
        rows = pl.ds(f * length_y, length_y)
        arrays = exchange([in_ref[r, rows] for r in range(ranks)], kept // ranks)
        for xh in range(hi):
            product = dot(table_ref[...], jnp.concatenate([arrays[xh], arrays[hi + xh]], 1))
            by_cos, by_sin = product[:length_y], product[length_y:]
            real = by_cos[:, :LANES] - by_sin[:, LANES:]
            imag = by_cos[:, LANES:] + by_sin[:, :LANES]
            out_ref[:, (f * 2) * hi + xh] = real.reshape(lo, cells_y, LANES)
            out_ref[:, (f * 2 + 1) * hi + xh] = imag.reshape(lo, cells_y, LANES)


def pool_matrix(rows, columns, weight, transposed):
    long_axis = 0 if transposed else 1
    shape = (columns, rows) if transposed else (rows, columns)
    long = lax.broadcasted_iota(jnp.int32, shape, long_axis)
    short = lax.broadcasted_iota(jnp.int32, shape, 1 - long_axis)
    return jnp.where(long // 2 == short, weight, 0.0).astype(jnp.float32)


def pool_rows(cells_x, cells_y):
    shape = (cells_x * cells_y // 4, cells_x * cells_y)
    short = lax.broadcasted_iota(jnp.int32, shape, 0)
    long = lax.broadcasted_iota(jnp.int32, shape, 1)
    same_x = long // (2 * cells_y) == short // (cells_y // 2)
    same_y = (long % cells_y) // 2 == short % (cells_y // 2)
    return jnp.where(same_x & same_y, 0.125, 0.0).astype(jnp.float32)


def z_back_kernel(sizes, in_ref, table_ref, modulus_ref, coarse_ref, held):
    lo, hi, kept = sizes
    cells_y = in_ref.shape[2]
    cells_x = lo * hi
    length_z = table_ref.shape[0]
    for xh in range(hi):
        tiles = {}
        for f in range(2):
            for c in range(2):
                arrays = [in_ref[p, (f * 2 + c) * hi + xh] for p in range(lo)]
                tiles[f, c] = exchange(arrays, kept)
        for xl in range(lo):
            mixed = swap_slot(tiles[0, 1][xl], tiles[1, 0][xl])
            members = ((tiles[0, 0][xl], mixed[0]), (mixed[1], tiles[1, 1][xl]))
            rows = pl.ds((xh * lo + xl) * cells_y, cells_y)
            for f in range(2):
                for c in range(2):
                    held[f, rows, pl.ds(c * LANES, LANES)] = members[f][c]
    coarse_ref[...] = jnp.zeros(coarse_ref.shape, jnp.float32)
    for f in range(2):
        values = jnp.exp(0.5 * dot(held[f], table_ref[...]))
        modulus_ref[f] = values.reshape(cells_x, cells_y, length_z)
        size_x, size_y, size_z = cells_x, cells_y, length_z
        start = 0
        for _ in range(3):
            right = pool_matrix(size_z // 2, size_z, 1.0, True)
            values = dot(pool_rows(size_x, size_y), dot(values, right))
            size_x, size_y, size_z = size_x // 2, size_y // 2, size_z // 2
            height = 2 * size_x * size_y // lo
            for d in range(lo // 2):
                piece = values[d * height : (d + 1) * height]
                place = (f * lo // 2 + d, pl.ds(start, height), pl.ds(0, size_z))
                coarse_ref[place] = piece
            start += height


def pick_kernel(heights, table_ref, in_ref, out_ref):
    for column in range(in_ref.shape[0]):
        start = 0
        for index, height in enumerate(heights):
            rows = pl.ds(start, height)
            out_ref[column, rows] = in_ref[table_ref[index, column], rows]
            start += height


def spread_kernel(axis, in_ref, out_ref, own_sem, send_sems, recv_sems):
    count = in_ref.shape[0]
    me = lax.axis_index(axis)
    barrier = pltpu.get_barrier_semaphore()
    for away in range(1, count):
        peer = lax.rem(me + away, count)
        pl.semaphore_signal(barrier, inc=1, device_id={axis: peer}, device_id_type=MESH)
    own = pltpu.make_async_copy(in_ref.at[me], out_ref.at[me], own_sem)
    own.start()
    pl.semaphore_wait(barrier, count - 1)
    copies = []
    for away in range(1, count):
        peer = lax.rem(me + away, count)
        copy = pltpu.make_async_remote_copy(
            src_ref=in_ref.at[peer],
            dst_ref=out_ref.at[me],
            send_sem=send_sems.at[away],
            recv_sem=recv_sems.at[away],
            device_id={axis: peer},
            device_id_type=MESH,
        )
        copy.start()
        copies.append(copy)
    own.wait()
    for copy in copies:
        copy.wait()


def spread_call(values, axis, number):
    count = values.shape[0]

    def body(*refs):
        spread_kernel(axis, *refs)

    return pl.pallas_call(
        body,
        out_shape=jax.ShapeDtypeStruct(values.shape, values.dtype),
        in_specs=[pl.BlockSpec(memory_space=pltpu.VMEM)],
        out_specs=pl.BlockSpec(memory_space=pltpu.VMEM),
        scratch_shapes=[
            pltpu.SemaphoreType.DMA,
            pltpu.SemaphoreType.DMA((count,)),
            pltpu.SemaphoreType.DMA((count,)),
        ],
        compiler_params=pltpu.CompilerParams(collective_id=number, has_side_effects=True),
    )(values)


def lanes_path(white_noise, spectrum, group_table):
    members, cells_x, cells_y, length_z = white_noise.shape
    size_px, size_py = lax.axis_size("px"), lax.axis_size("py")
    length_x, length_y = cells_x * size_px, cells_y * size_py
    lo, hi = size_py, cells_x // size_py
    kept = LANES // size_py
    sizes = (lo, hi, kept)
    f32 = jnp.float32
    params = pltpu.CompilerParams(vmem_limit_bytes=48 * 1024 * 1024)

    def call(body, shapes, *operands, scratch=(), scalars=0):
        out = [jax.ShapeDtypeStruct(shape, f32) for shape in shapes]
        specs = [pl.BlockSpec(memory_space=pltpu.SMEM)] * scalars
        specs += [pl.BlockSpec(memory_space=pltpu.VMEM)] * (len(operands) - scalars)
        return pl.pallas_call(
            body,
            out_shape=out,
            in_specs=specs,
            out_specs=[pl.BlockSpec(memory_space=pltpu.VMEM)] * len(out),
            scratch_shapes=list(scratch),
            compiler_params=params,
        )(*operands)

    z_ahead, z_back = half_tables(length_z)
    z_ahead = z_ahead.reshape(length_z, length_z)
    z_back = z_back.reshape(length_z, length_z).T * (1.0 / (length_x * length_y * length_z))
    angles = angles_of(length_y)
    y_table = jnp.asarray(np.concatenate([np.cos(angles), np.sin(angles)], 0), f32)
    lane = np.arange(LANES)
    part = (lane // (hi * size_px)) % 2
    place = (lane % size_px) * cells_x + (lane // size_px % hi) * lo + lane // kept

    def x_table(direction):
        table = complex_array(length_x, direction)
        rows = table[part, place]
        return jnp.asarray(rows[:, part, place], f32)

    first = (lax.axis_index("px") == 0) & (lax.axis_index("py") == 0)
    first = first.astype(jnp.int32).reshape(1)
    held = pltpu.VMEM((members, cells_x * cells_y, length_z), f32)

    def bind(body):
        def bound(*refs):
            body(sizes, *refs)

        return bound

    tiles = 4 * hi
    (values,) = call(
        bind(z_forward_kernel),
        [(size_py, tiles + hi + 1, cells_y, LANES)],
        white_noise,
        spectrum,
        z_ahead,
        scratch=[held],
    )
    values = spread_call(values, "py", 0)
    (values,) = call(
        bind(y_forward_kernel), [(size_px, 3 * length_y, LANES)], values, y_table
    )
    values = spread_call(values, "px", 1)
    (values,) = call(
        bind(x_kernel),
        [(size_px, 2 * length_y, LANES)],
        first,
        values,
        x_table(-1.0),
        x_table(1.0),
        scalars=1,
    )
    values = spread_call(values, "px", 2)
    (values,) = call(
        bind(y_back_kernel), [(size_py, tiles, cells_y, LANES)], values, y_table
    )
    values = spread_call(values, "py", 3)
    shapes = []
    heights = []
    size = (cells_x, cells_y, length_z)
    for _ in range(3):
        size = tuple(extent // 2 for extent in size)
        shapes.append((members,) + size)
        heights.append(members * size[0] * size[1] // size_py)
    modulus, coarse = call(
        bind(z_back_kernel),
        [white_noise.shape, (size_py, sum(heights), LANES)],
        values,
        z_back,
        scratch=[held],
    )
    coarse = spread_call(coarse, "py", 4)

    def pick(*refs):
        pick_kernel(heights, *refs)

    (coarse,) = call(pick, [coarse.shape], group_table, coarse, scalars=1)
    coarse = spread_call(coarse, "py", 5)
    routed, start = [], 0
    for shape, height in zip(shapes, heights):
        routed.append(coarse[:, start : start + height, : shape[3]].reshape(shape))
        start += height
    return (modulus, routed[0], routed[1], routed[2])


def on_device(white_noise, spectrum, group_table):
    members, cells_x, cells_y, length_z = white_noise.shape
    size_px, size_py = lax.axis_size("px"), lax.axis_size("py")
    fits = members == 2 and length_z == 2 * LANES and 2 * cells_x * size_px == LANES
    fits = fits and cells_x * 2 == size_px * size_py
    fits = fits and size_px * size_px * size_py == LANES
    chosen = lanes_path if fits else general_path
    return chosen(white_noise, spectrum, group_table)


def solution(mesh):
    in_specs = (P(None, "px", "py", None), P("px", "py", None), P())
    out_specs = (P(None, "px", "py", None),) * 4
    return jax.shard_map(
        on_device, mesh=mesh, in_specs=in_specs, out_specs=out_specs, check_vma=False
    )
```

```python
import numpy as np

import jax
import jax.numpy as jnp
from jax import lax
from jax.experimental import pallas as pl
from jax.experimental.pallas import tpu as pltpu
from jax.sharding import PartitionSpec as P


def angles_of(length):
    positions = np.arange(length, dtype=np.int64)
    return (positions[:, None] * positions[None, :] % length) * (2.0 * np.pi / length)


def complex_array(length, direction):
    angles = angles_of(length)
    cos, sin = np.cos(angles), direction * np.sin(angles)
    return np.stack([np.stack([cos, sin], 1), np.stack([-sin, cos], 1)], 0)


def complex_table(length, direction):
    return jnp.asarray(complex_array(length, direction), jnp.float32)


def half_tables(length):
    angles = angles_of(length)[:, : length // 2]
    ahead = np.stack([np.cos(angles), -np.sin(angles)], 1)
    back = 2.0 * ahead
    nyquist = np.where(np.arange(length) % 2 == 0, 1.0, -1.0)
    ahead[:, 1, 0] = nyquist
    back[:, 0, 0] = 1.0
    back[:, 1, 0] = nyquist
    return jnp.asarray(ahead, jnp.float32), jnp.asarray(back, jnp.float32)


def einsum(pattern, left, right):
    return jnp.einsum(pattern, left, right, precision=lax.Precision.HIGH)


def swap_first(values):
    first = values[:, :, :1]
    turned = jnp.swapaxes(first, 0, 1)
    return jnp.concatenate([turned, values[:, :, 1:]], 2)


def coarsen(values):
    members, size_x, size_y, size_z = values.shape
    blocks = values.reshape(members, size_x // 2, 2, size_y // 2, 2, size_z // 2, 2)
    return blocks.mean(axis=(2, 4, 6))


def general_path(white_noise, spectrum, group_table):
    members, cells_x, cells_y, length_z = white_noise.shape
    size_px, size_py = lax.axis_size("px"), lax.axis_size("py")
    length_x, length_y = cells_x * size_px, cells_y * size_py
    half_z = length_z // 2
    block_py, block = half_z // size_py, half_z // size_py // size_px
    z_ahead, z_back = half_tables(length_z)
    scale = 1.0 / (length_x * length_y * length_z)

    table = jnp.transpose(spectrum, (2, 0, 1))
    last = jnp.broadcast_to(table[half_z : half_z + 1], (size_py, 1, cells_x, cells_y))
    table = jnp.concatenate([table[:half_z].reshape(size_py, block_py, cells_x, cells_y), last], 1)
    table = lax.all_to_all(table, "py", split_axis=0, concat_axis=3, tiled=True)[0]
    last = jnp.broadcast_to(table[block_py:], (size_px, 1, cells_x, length_y))
    table = jnp.concatenate([table[:block_py].reshape(size_px, block, cells_x, length_y), last], 1)
    table = lax.all_to_all(table, "px", split_axis=0, concat_axis=2, tiled=True)[0] * scale
    is_first = (lax.axis_index("px") == 0) & (lax.axis_index("py") == 0)
    other = jnp.where(is_first, table[block:], table[:1])
    tables = jnp.stack([table[:block], jnp.concatenate([other, table[1:block]], 0)], 0)

    values = einsum("fxyz,zck->fckxy", white_noise, z_ahead)
    values = swap_first(values)
    values = lax.all_to_all(values, "py", split_axis=2, concat_axis=4, tiled=True)
    values = einsum("fckxy,cydm->fdkxm", values, complex_table(length_y, -1.0))
    values = lax.all_to_all(values, "px", split_axis=2, concat_axis=3, tiled=True)
    values = einsum("fckxm,cxdj->fdkjm", values, complex_table(length_x, -1.0))
    values = values * tables[:, None]
    values = einsum("fckjm,cjdx->fdkxm", values, complex_table(length_x, 1.0))
    values = lax.all_to_all(values, "px", split_axis=3, concat_axis=2, tiled=True)
    values = einsum("fckxm,cmdy->fdkxy", values, complex_table(length_y, 1.0))
    values = lax.all_to_all(values, "py", split_axis=4, concat_axis=2, tiled=True)
    values = swap_first(values)
    fields = einsum("fckxy,zck->fxyz", values, z_back)
    modulus = jnp.exp(0.5 * fields)

    levels = []
    level = modulus
    for _ in range(3):
        level = coarsen(level)
        levels.append(level)
    pieces = [jnp.reshape(level, (size_py, -1)) for level in levels]
    widths = [piece.shape[1] for piece in pieces]
    joined = jnp.concatenate(pieces, 1)
    spread = lax.all_to_all(joined, "py", split_axis=0, concat_axis=0, tiled=True)
    picked, start = [], 0
    for index, width in enumerate(widths):
        part = spread[:, start : start + width]
        picked.append(jnp.take(part, group_table[index], axis=0))
        start += width
    joined = lax.all_to_all(
        jnp.concatenate(picked, 1), "py", split_axis=0, concat_axis=0, tiled=True
    )
    routed, start = [], 0
    for level, width in zip(levels, widths):
        routed.append(joined[:, start : start + width].reshape(level.shape))
        start += width
    return (modulus, routed[0], routed[1], routed[2])


LANES = 128
MESH = pl.DeviceIdType.MESH


def dot(left, right):
    return jnp.dot(
        left, right, precision=lax.Precision.HIGHEST, preferred_element_type=jnp.float32
    )


def lane_of(shape):
    return lax.broadcasted_iota(jnp.int32, shape, len(shape) - 1)


def exchange(arrays, width):
    arrays = list(arrays)
    lane = lane_of(arrays[0].shape)
    distance = 1
    while distance < len(arrays):
        step = distance * width
        low = (lane // step) % 2 == 0
        for index in range(len(arrays)):
            if (index // distance) % 2 == 0:
                first, second = arrays[index], arrays[index + distance]
                arrays[index] = jnp.where(low, first, pltpu.roll(second, step, 1))
                arrays[index + distance] = jnp.where(
                    low, pltpu.roll(first, LANES - step, 1), second
                )
        distance *= 2
    return arrays


def swap_slot(first, second):
    at_zero = lane_of(first.shape) == 0
    return jnp.where(at_zero, second, first), jnp.where(at_zero, first, second)


def z_forward_kernel(sizes, noise_ref, spectrum_ref, table_ref, out_ref, held):
    lo, hi, kept = sizes
    cells_y = noise_ref.shape[2]
    for f in range(2):
        rows = noise_ref[f].reshape(lo * hi * cells_y, noise_ref.shape[3])
        held[f] = dot(rows, table_ref[...])

    def tile(f, c, x):
        return held[f, pl.ds(x * cells_y, cells_y), pl.ds(c * LANES, LANES)]

    for xh in range(hi):
        tiles = {}
        for xl in range(lo):
            x = xh * lo + xl
            mixed = swap_slot(tile(0, 1, x), tile(1, 0, x))
            members = ((tile(0, 0, x), mixed[0]), (mixed[1], tile(1, 1, x)))
            for f in range(2):
                for c in range(2):
                    tiles[f, c, xl] = members[f][c]
        for f in range(2):
            for c in range(2):
                moved = exchange([tiles[f, c, xl] for xl in range(lo)], kept)
                for p in range(lo):
                    out_ref[p, (f * 2 + c) * hi + xh] = moved[p]
    group = lane_of((cells_y, LANES))
    last = jnp.zeros((cells_y, LANES), jnp.float32)
    for xh in range(hi):
        names = [xh * lo + xl for xl in range(lo)]
        moved = exchange([spectrum_ref[x, :, pl.ds(0, LANES)] for x in names], kept)
        for p in range(lo):
            out_ref[p, 4 * hi + xh] = moved[p]
        for xl in range(lo):
            value = spectrum_ref[names[xl], :, pl.ds(LANES, 1)]
            last = jnp.where(group == xl * kept + xh, value, last)
    for p in range(lo):
        out_ref[p, 5 * hi] = last


def y_forward_kernel(sizes, in_ref, table_ref, out_ref):
    lo, hi, kept = sizes
    length_y = table_ref.shape[1]
    ranks = 2 * hi
    half = length_y // 2

    def whole(t):
        return in_ref[:, t].reshape(length_y, LANES)

    for f in range(2):
        arrays = [None] * ranks
        for xh in range(hi):
            pair = [whole((f * 2 + c) * hi + xh) for c in range(2)]
            product = dot(table_ref[...], jnp.concatenate(pair, 1))
            by_cos, by_sin = product[:length_y], product[length_y:]
            arrays[xh] = by_cos[:, :LANES] + by_sin[:, LANES:]
            arrays[hi + xh] = by_cos[:, LANES:] - by_sin[:, :LANES]
        moved = exchange(arrays, kept // ranks)
        for r in range(ranks):
            out_ref[r, pl.ds(f * length_y, length_y)] = moved[r]
    halves = []
    for mh in range(2):
        for xh in range(hi):
            halves.append(whole(4 * hi + xh)[mh * half : (mh + 1) * half])
    moved = exchange(halves, kept // ranks)
    last = whole(5 * hi)
    packed = last[:half] + pltpu.roll(last[half:], hi, 1)
    for r in range(ranks):
        out_ref[r, pl.ds(2 * length_y, half)] = moved[r]
        out_ref[r, pl.ds(2 * length_y + half, half)] = packed


def x_kernel(sizes, first_ref, in_ref, ahead_ref, back_ref, out_ref):
    lo, hi, kept = sizes
    ranks = 2 * hi
    length_y = out_ref.shape[1] // 2
    half = length_y // 2
    lane = lane_of((half, LANES))
    low = (lane // (hi * ranks)) % 2 == 0
    parts = [in_ref[r, pl.ds(2 * length_y, half)] for r in range(ranks)]
    tables = []
    for part in exchange(parts, 1):
        upper = jnp.where(low, part, pltpu.roll(part, hi * ranks, 1))
        lower = jnp.where(low, pltpu.roll(part, LANES - hi * ranks, 1), part)
        tables.append(jnp.concatenate([upper, lower], 0))
    last = [in_ref[r, pl.ds(2 * length_y + half, half)] for r in range(ranks)]
    last = jnp.concatenate(last, 1)
    source = lax.broadcasted_iota(jnp.int32, (ranks * LANES, LANES), 0)
    target = lax.broadcasted_iota(jnp.int32, (ranks * LANES, LANES), 1)
    same = (source // LANES == target % ranks) & ((source % LANES) // kept == target // kept)
    level = (target // ranks) % hi
    picked = []
    for mh in range(2):
        chosen = same & (source % kept == mh * hi + level)
        picked.append(dot(last, chosen.astype(jnp.float32)))
    last = jnp.concatenate(picked, 0)
    is_first = lax.broadcasted_iota(jnp.int32, last.shape, 0) * 0 + first_ref[0] == 1
    other = jnp.where(is_first, last, tables[0])
    for f in range(2):
        rows = pl.ds(f * length_y, length_y)
        arrays = exchange([in_ref[r, rows] for r in range(ranks)], 1)
        for q in range(ranks):
            table = other if f == 1 and q == 0 else tables[q]
            arrays[q] = dot(dot(arrays[q], ahead_ref[...]) * table, back_ref[...])
        arrays = exchange(arrays, 1)
        for r in range(ranks):
            out_ref[r, rows] = arrays[r]


def y_back_kernel(sizes, in_ref, table_ref, out_ref):
    lo, hi, kept = sizes
    ranks = 2 * hi
    length_y = table_ref.shape[1]
    cells_y = length_y // lo
    for f in range(2):
        rows = pl.ds(f * length_y, length_y)
        arrays = exchange([in_ref[r, rows] for r in range(ranks)], kept // ranks)
        for xh in range(hi):
            product = dot(table_ref[...], jnp.concatenate([arrays[xh], arrays[hi + xh]], 1))
            by_cos, by_sin = product[:length_y], product[length_y:]
            real = by_cos[:, :LANES] - by_sin[:, LANES:]
            imag = by_cos[:, LANES:] + by_sin[:, :LANES]
            out_ref[:, (f * 2) * hi + xh] = real.reshape(lo, cells_y, LANES)
            out_ref[:, (f * 2 + 1) * hi + xh] = imag.reshape(lo, cells_y, LANES)


def pool_matrix(rows, columns, weight, transposed):
    long_axis = 0 if transposed else 1
    shape = (columns, rows) if transposed else (rows, columns)
    long = lax.broadcasted_iota(jnp.int32, shape, long_axis)
    short = lax.broadcasted_iota(jnp.int32, shape, 1 - long_axis)
    return jnp.where(long // 2 == short, weight, 0.0).astype(jnp.float32)


def pool_rows(cells_x, cells_y):
    shape = (cells_x * cells_y // 4, cells_x * cells_y)
    short = lax.broadcasted_iota(jnp.int32, shape, 0)
    long = lax.broadcasted_iota(jnp.int32, shape, 1)
    same_x = long // (2 * cells_y) == short // (cells_y // 2)
    same_y = (long % cells_y) // 2 == short % (cells_y // 2)
    return jnp.where(same_x & same_y, 0.125, 0.0).astype(jnp.float32)


def z_back_kernel(sizes, in_ref, table_ref, modulus_ref, coarse_ref, held):
    lo, hi, kept = sizes
    cells_y = in_ref.shape[2]
    cells_x = lo * hi
    length_z = table_ref.shape[0]
    for xh in range(hi):
        tiles = {}
        for f in range(2):
            for c in range(2):
                arrays = [in_ref[p, (f * 2 + c) * hi + xh] for p in range(lo)]
                tiles[f, c] = exchange(arrays, kept)
        for xl in range(lo):
            mixed = swap_slot(tiles[0, 1][xl], tiles[1, 0][xl])
            members = ((tiles[0, 0][xl], mixed[0]), (mixed[1], tiles[1, 1][xl]))
            rows = pl.ds((xh * lo + xl) * cells_y, cells_y)
            for f in range(2):
                for c in range(2):
                    held[f, rows, pl.ds(c * LANES, LANES)] = members[f][c]
    coarse_ref[...] = jnp.zeros(coarse_ref.shape, jnp.float32)
    for f in range(2):
        values = jnp.exp(0.5 * dot(held[f], table_ref[...]))
        modulus_ref[f] = values.reshape(cells_x, cells_y, length_z)
        size_x, size_y, size_z = cells_x, cells_y, length_z
        start = 0
        for _ in range(3):
            right = pool_matrix(size_z // 2, size_z, 1.0, True)
            values = dot(pool_rows(size_x, size_y), dot(values, right))
            size_x, size_y, size_z = size_x // 2, size_y // 2, size_z // 2
            height = 2 * size_x * size_y // lo
            for d in range(lo // 2):
                piece = values[d * height : (d + 1) * height]
                place = (f * lo // 2 + d, pl.ds(start, height), pl.ds(0, size_z))
                coarse_ref[place] = piece
            start += height


def pick_kernel(heights, table_ref, in_ref, out_ref):
    for column in range(in_ref.shape[0]):
        start = 0
        for index, height in enumerate(heights):
            rows = pl.ds(start, height)
            out_ref[column, rows] = in_ref[table_ref[index, column], rows]
            start += height


def spread_kernel(axis, tail, used, in_ref, out_ref, own_sem, sends, recvs, tail_sends, tail_recvs):
    count, height = in_ref.shape[0], in_ref.shape[1]
    me = lax.axis_index(axis)
    used = used()
    rest = pl.ds(tail, height - tail)
    barrier = pltpu.get_barrier_semaphore()
    for away in range(1, count):
        peer = lax.rem(me + away, count)
        pl.semaphore_signal(barrier, inc=1, device_id={axis: peer}, device_id_type=MESH)
    own = pltpu.make_async_copy(in_ref.at[me], out_ref.at[me], own_sem)
    own.start()
    pl.semaphore_wait(barrier, count - 1)
    copies, extras = [], []
    for away in range(1, count):
        peer = lax.rem(me + away, count)
        copy = pltpu.make_async_remote_copy(
            src_ref=in_ref.at[peer, pl.ds(0, tail)],
            dst_ref=out_ref.at[me, pl.ds(0, tail)],
            send_sem=sends.at[away],
            recv_sem=recvs.at[away],
            device_id={axis: peer},
            device_id_type=MESH,
        )
        copy.start()
        copies.append(copy)
    for source in range(1, count):
        extra = pltpu.make_async_remote_copy(
            src_ref=in_ref.at[0, rest],
            dst_ref=out_ref.at[source, rest],
            send_sem=tail_sends.at[source],
            recv_sem=tail_recvs.at[source],
            device_id={axis: 0},
            device_id_type=MESH,
        )
        pl.when((me == source) & used)(extra.start)
        extras.append(extra)
    for source in range(count):

        @pl.when((me != source) & jnp.logical_not((me == 0) & used))
        def _():
            out_ref[source, rest] = jnp.zeros(out_ref.shape[1:], jnp.float32)[tail:]

    own.wait()
    for copy in copies:
        copy.wait()
    for source in range(1, count):
        pl.when((me == source) & used)(extras[source - 1].wait_send)
        pl.when((me == 0) & used)(extras[source - 1].wait_recv)


def spread_call(values, axis, number, tail, used):
    count = values.shape[0]

    def body(*refs):
        spread_kernel(axis, tail, used, *refs)

    return pl.pallas_call(
        body,
        out_shape=jax.ShapeDtypeStruct(values.shape, values.dtype),
        in_specs=[pl.BlockSpec(memory_space=pltpu.VMEM)],
        out_specs=pl.BlockSpec(memory_space=pltpu.VMEM),
        scratch_shapes=[pltpu.SemaphoreType.DMA] + [pltpu.SemaphoreType.DMA((count,))] * 4,
        compiler_params=pltpu.CompilerParams(collective_id=number, has_side_effects=True),
    )(values)


def spread(values, axis):
    return lax.all_to_all(values, axis, split_axis=0, concat_axis=0, tiled=True)


def lanes_path(white_noise, spectrum, group_table):
    members, cells_x, cells_y, length_z = white_noise.shape
    size_px, size_py = lax.axis_size("px"), lax.axis_size("py")
    length_x, length_y = cells_x * size_px, cells_y * size_py
    lo, hi = size_py, cells_x // size_py
    kept = LANES // size_py
    sizes = (lo, hi, kept)
    f32 = jnp.float32
    params = pltpu.CompilerParams(vmem_limit_bytes=48 * 1024 * 1024)

    def call(body, shapes, *operands, scratch=(), scalars=0):
        out = [jax.ShapeDtypeStruct(shape, f32) for shape in shapes]
        specs = [pl.BlockSpec(memory_space=pltpu.SMEM)] * scalars
        specs += [pl.BlockSpec(memory_space=pltpu.VMEM)] * (len(operands) - scalars)
        return pl.pallas_call(
            body,
            out_shape=out,
            in_specs=specs,
            out_specs=[pl.BlockSpec(memory_space=pltpu.VMEM)] * len(out),
            scratch_shapes=list(scratch),
            compiler_params=params,
        )(*operands)

    z_ahead, z_back = half_tables(length_z)
    z_ahead = z_ahead.reshape(length_z, length_z)
    z_back = z_back.reshape(length_z, length_z).T * (1.0 / (length_x * length_y * length_z))
    angles = angles_of(length_y)
    y_table = jnp.asarray(np.concatenate([np.cos(angles), np.sin(angles)], 0), f32)
    lane = np.arange(LANES)
    part = (lane // (hi * size_px)) % 2
    place = (lane % size_px) * cells_x + (lane // size_px % hi) * lo + lane // kept

    def x_table(direction):
        table = complex_array(length_x, direction)
        rows = table[part, place]
        return jnp.asarray(rows[:, part, place], f32)

    first = (lax.axis_index("px") == 0) & (lax.axis_index("py") == 0)
    first = first.astype(jnp.int32).reshape(1)
    held = pltpu.VMEM((members, cells_x * cells_y, length_z), f32)

    def bind(body):
        def bound(*refs):
            body(sizes, *refs)

        return bound

    tiles = 4 * hi
    (values,) = call(
        bind(z_forward_kernel),
        [(size_py, tiles + hi + 1, cells_y, LANES)],
        white_noise,
        spectrum,
        z_ahead,
        scratch=[held],
    )
    values = spread_call(values, "py", 0, tiles + hi, lambda: True)
    (values,) = call(
        bind(y_forward_kernel), [(size_px, 3 * length_y, LANES)], values, y_table
    )
    values = spread_call(
        values, "px", 1, 2 * length_y + length_y // 2, lambda: lax.axis_index("py") == 0
    )
    (values,) = call(
        bind(x_kernel),
        [(size_px, 2 * length_y, LANES)],
        first,
        values,
        x_table(-1.0),
        x_table(1.0),
        scalars=1,
    )
    values = spread(values, "px")
    (values,) = call(
        bind(y_back_kernel), [(size_py, tiles, cells_y, LANES)], values, y_table
    )
    values = spread(values, "py")
    shapes = []
    heights = []
    size = (cells_x, cells_y, length_z)
    for _ in range(3):
        size = tuple(extent // 2 for extent in size)
        shapes.append((members,) + size)
        heights.append(members * size[0] * size[1] // size_py)
    modulus, coarse = call(
        bind(z_back_kernel),
        [white_noise.shape, (size_py, sum(heights), LANES)],
        values,
        z_back,
        scratch=[held],
    )
    coarse = spread(coarse, "py")

    def pick(*refs):
        pick_kernel(heights, *refs)

    (coarse,) = call(pick, [coarse.shape], group_table, coarse, scalars=1)
    coarse = spread(coarse, "py")
    routed, start = [], 0
    for shape, height in zip(shapes, heights):
        routed.append(coarse[:, start : start + height, : shape[3]].reshape(shape))
        start += height
    return (modulus, routed[0], routed[1], routed[2])


def on_device(white_noise, spectrum, group_table):
    members, cells_x, cells_y, length_z = white_noise.shape
    size_px, size_py = lax.axis_size("px"), lax.axis_size("py")
    fits = members == 2 and length_z == 2 * LANES and 2 * cells_x * size_px == LANES
    fits = fits and cells_x * 2 == size_px * size_py
    fits = fits and size_px * size_px * size_py == LANES
    chosen = lanes_path if fits else general_path
    return chosen(white_noise, spectrum, group_table)


def solution(mesh):
    in_specs = (P(None, "px", "py", None), P("px", "py", None), P())
    out_specs = (P(None, "px", "py", None),) * 4
    return jax.shard_map(
        on_device, mesh=mesh, in_specs=in_specs, out_specs=out_specs, check_vma=False
    )
```

```python
import numpy as np

import jax
import jax.numpy as jnp
from jax import lax
from jax.experimental import pallas as pl
from jax.experimental.pallas import tpu as pltpu
from jax.sharding import PartitionSpec as P


def angles_of(length):
    positions = np.arange(length, dtype=np.int64)
    return (positions[:, None] * positions[None, :] % length) * (2.0 * np.pi / length)


def complex_array(length, direction):
    angles = angles_of(length)
    cos, sin = np.cos(angles), direction * np.sin(angles)
    return np.stack([np.stack([cos, sin], 1), np.stack([-sin, cos], 1)], 0)


def complex_table(length, direction):
    return jnp.asarray(complex_array(length, direction), jnp.float32)


def half_tables(length):
    angles = angles_of(length)[:, : length // 2]
    ahead = np.stack([np.cos(angles), -np.sin(angles)], 1)
    back = 2.0 * ahead
    nyquist = np.where(np.arange(length) % 2 == 0, 1.0, -1.0)
    ahead[:, 1, 0] = nyquist
    back[:, 0, 0] = 1.0
    back[:, 1, 0] = nyquist
    return jnp.asarray(ahead, jnp.float32), jnp.asarray(back, jnp.float32)


def einsum(pattern, left, right):
    return jnp.einsum(pattern, left, right, precision=lax.Precision.HIGH)


def swap_first(values):
    first = values[:, :, :1]
    turned = jnp.swapaxes(first, 0, 1)
    return jnp.concatenate([turned, values[:, :, 1:]], 2)


def coarsen(values):
    members, size_x, size_y, size_z = values.shape
    blocks = values.reshape(members, size_x // 2, 2, size_y // 2, 2, size_z // 2, 2)
    return blocks.mean(axis=(2, 4, 6))


def general_path(white_noise, spectrum, group_table):
    members, cells_x, cells_y, length_z = white_noise.shape
    size_px, size_py = lax.axis_size("px"), lax.axis_size("py")
    length_x, length_y = cells_x * size_px, cells_y * size_py
    half_z = length_z // 2
    block_py, block = half_z // size_py, half_z // size_py // size_px
    z_ahead, z_back = half_tables(length_z)
    scale = 1.0 / (length_x * length_y * length_z)

    table = jnp.transpose(spectrum, (2, 0, 1))
    last = jnp.broadcast_to(table[half_z : half_z + 1], (size_py, 1, cells_x, cells_y))
    table = jnp.concatenate([table[:half_z].reshape(size_py, block_py, cells_x, cells_y), last], 1)
    table = lax.all_to_all(table, "py", split_axis=0, concat_axis=3, tiled=True)[0]
    last = jnp.broadcast_to(table[block_py:], (size_px, 1, cells_x, length_y))
    table = jnp.concatenate([table[:block_py].reshape(size_px, block, cells_x, length_y), last], 1)
    table = lax.all_to_all(table, "px", split_axis=0, concat_axis=2, tiled=True)[0] * scale
    is_first = (lax.axis_index("px") == 0) & (lax.axis_index("py") == 0)
    other = jnp.where(is_first, table[block:], table[:1])
    tables = jnp.stack([table[:block], jnp.concatenate([other, table[1:block]], 0)], 0)

    values = einsum("fxyz,zck->fckxy", white_noise, z_ahead)
    values = swap_first(values)
    values = lax.all_to_all(values, "py", split_axis=2, concat_axis=4, tiled=True)
    values = einsum("fckxy,cydm->fdkxm", values, complex_table(length_y, -1.0))
    values = lax.all_to_all(values, "px", split_axis=2, concat_axis=3, tiled=True)
    values = einsum("fckxm,cxdj->fdkjm", values, complex_table(length_x, -1.0))
    values = values * tables[:, None]
    values = einsum("fckjm,cjdx->fdkxm", values, complex_table(length_x, 1.0))
    values = lax.all_to_all(values, "px", split_axis=3, concat_axis=2, tiled=True)
    values = einsum("fckxm,cmdy->fdkxy", values, complex_table(length_y, 1.0))
    values = lax.all_to_all(values, "py", split_axis=4, concat_axis=2, tiled=True)
    values = swap_first(values)
    fields = einsum("fckxy,zck->fxyz", values, z_back)
    modulus = jnp.exp(0.5 * fields)

    levels = []
    level = modulus
    for _ in range(3):
        level = coarsen(level)
        levels.append(level)
    pieces = [jnp.reshape(level, (size_py, -1)) for level in levels]
    widths = [piece.shape[1] for piece in pieces]
    joined = jnp.concatenate(pieces, 1)
    spread = lax.all_to_all(joined, "py", split_axis=0, concat_axis=0, tiled=True)
    picked, start = [], 0
    for index, width in enumerate(widths):
        part = spread[:, start : start + width]
        picked.append(jnp.take(part, group_table[index], axis=0))
        start += width
    joined = lax.all_to_all(
        jnp.concatenate(picked, 1), "py", split_axis=0, concat_axis=0, tiled=True
    )
    routed, start = [], 0
    for level, width in zip(levels, widths):
        routed.append(joined[:, start : start + width].reshape(level.shape))
        start += width
    return (modulus, routed[0], routed[1], routed[2])


LANES = 128
MESH = pl.DeviceIdType.MESH


def dot(left, right):
    return jnp.dot(
        left, right, precision=lax.Precision.HIGHEST, preferred_element_type=jnp.float32
    )


def lane_of(shape):
    return lax.broadcasted_iota(jnp.int32, shape, len(shape) - 1)


def exchange(arrays, width):
    arrays = list(arrays)
    lane = lane_of(arrays[0].shape)
    distance = 1
    while distance < len(arrays):
        step = distance * width
        low = (lane // step) % 2 == 0
        for index in range(len(arrays)):
            if (index // distance) % 2 == 0:
                first, second = arrays[index], arrays[index + distance]
                arrays[index] = jnp.where(low, first, pltpu.roll(second, step, 1))
                arrays[index + distance] = jnp.where(
                    low, pltpu.roll(first, LANES - step, 1), second
                )
        distance *= 2
    return arrays


def swap_slot(first, second):
    at_zero = lane_of(first.shape) == 0
    return jnp.where(at_zero, second, first), jnp.where(at_zero, first, second)


def z_forward_kernel(sizes, noise_ref, spectrum_ref, table_ref, out_ref, held):
    lo, hi, kept = sizes
    cells_y = noise_ref.shape[2]
    for f in range(2):
        rows = noise_ref[f].reshape(lo * hi * cells_y, noise_ref.shape[3])
        held[f] = dot(rows, table_ref[...])

    def tile(f, c, x):
        return held[f, pl.ds(x * cells_y, cells_y), pl.ds(c * LANES, LANES)]

    for xh in range(hi):
        tiles = {}
        for xl in range(lo):
            x = xh * lo + xl
            mixed = swap_slot(tile(0, 1, x), tile(1, 0, x))
            members = ((tile(0, 0, x), mixed[0]), (mixed[1], tile(1, 1, x)))
            for f in range(2):
                for c in range(2):
                    tiles[f, c, xl] = members[f][c]
        for f in range(2):
            for c in range(2):
                moved = exchange([tiles[f, c, xl] for xl in range(lo)], kept)
                for p in range(lo):
                    out_ref[p, (f * 2 + c) * hi + xh] = moved[p]
    group = lane_of((cells_y, LANES))
    last = jnp.zeros((cells_y, LANES), jnp.float32)
    for xh in range(hi):
        names = [xh * lo + xl for xl in range(lo)]
        moved = exchange([spectrum_ref[x, :, pl.ds(0, LANES)] for x in names], kept)
        for p in range(lo):
            out_ref[p, 4 * hi + xh] = moved[p]
        for xl in range(lo):
            value = spectrum_ref[names[xl], :, pl.ds(LANES, 1)]
            last = jnp.where(group == xl * kept + xh, value, last)
    for p in range(lo):
        out_ref[p, 5 * hi] = last


def y_forward_kernel(sizes, in_ref, table_ref, out_ref):
    lo, hi, kept = sizes
    length_y = table_ref.shape[1]
    ranks = 2 * hi
    half = length_y // 2

    def whole(t):
        return in_ref[:, t].reshape(length_y, LANES)

    for f in range(2):
        arrays = [None] * ranks
        for xh in range(hi):
            pair = [whole((f * 2 + c) * hi + xh) for c in range(2)]
            product = dot(table_ref[...], jnp.concatenate(pair, 1))
            by_cos, by_sin = product[:length_y], product[length_y:]
            arrays[xh] = by_cos[:, :LANES] + by_sin[:, LANES:]
            arrays[hi + xh] = by_cos[:, LANES:] - by_sin[:, :LANES]
        moved = exchange(arrays, kept // ranks)
        for r in range(ranks):
            out_ref[r, pl.ds(f * length_y, length_y)] = moved[r]
    halves = []
    for mh in range(2):
        for xh in range(hi):
            halves.append(whole(4 * hi + xh)[mh * half : (mh + 1) * half])
    moved = exchange(halves, kept // ranks)
    last = whole(5 * hi)
    packed = last[:half] + pltpu.roll(last[half:], hi, 1)
    for r in range(ranks):
        out_ref[r, pl.ds(2 * length_y, half)] = moved[r]
        out_ref[r, pl.ds(2 * length_y + half, half)] = packed


def x_kernel(sizes, first_ref, in_ref, ahead_ref, back_ref, out_ref):
    lo, hi, kept = sizes
    ranks = 2 * hi
    length_y = out_ref.shape[1] // 2
    half = length_y // 2
    lane = lane_of((half, LANES))
    low = (lane // (hi * ranks)) % 2 == 0
    parts = [in_ref[r, pl.ds(2 * length_y, half)] for r in range(ranks)]
    tables = []
    for part in exchange(parts, 1):
        upper = jnp.where(low, part, pltpu.roll(part, hi * ranks, 1))
        lower = jnp.where(low, pltpu.roll(part, LANES - hi * ranks, 1), part)
        tables.append(jnp.concatenate([upper, lower], 0))
    last = [in_ref[r, pl.ds(2 * length_y + half, half)] for r in range(ranks)]
    last = jnp.concatenate(last, 1)
    source = lax.broadcasted_iota(jnp.int32, (ranks * LANES, LANES), 0)
    target = lax.broadcasted_iota(jnp.int32, (ranks * LANES, LANES), 1)
    same = (source // LANES == target % ranks) & ((source % LANES) // kept == target // kept)
    level = (target // ranks) % hi
    picked = []
    for mh in range(2):
        chosen = same & (source % kept == mh * hi + level)
        picked.append(dot(last, chosen.astype(jnp.float32)))
    last = jnp.concatenate(picked, 0)
    is_first = lax.broadcasted_iota(jnp.int32, last.shape, 0) * 0 + first_ref[0] == 1
    other = jnp.where(is_first, last, tables[0])
    for f in range(2):
        rows = pl.ds(f * length_y, length_y)
        arrays = exchange([in_ref[r, rows] for r in range(ranks)], 1)
        for q in range(ranks):
            table = other if f == 1 and q == 0 else tables[q]
            arrays[q] = dot(dot(arrays[q], ahead_ref[...]) * table, back_ref[...])
        arrays = exchange(arrays, 1)
        for r in range(ranks):
            out_ref[r, rows] = arrays[r]


def y_back_kernel(sizes, in_ref, table_ref, out_ref):
    lo, hi, kept = sizes
    ranks = 2 * hi
    length_y = table_ref.shape[1]
    cells_y = length_y // lo
    for f in range(2):
        rows = pl.ds(f * length_y, length_y)
        arrays = exchange([in_ref[r, rows] for r in range(ranks)], kept // ranks)
        for xh in range(hi):
            product = dot(table_ref[...], jnp.concatenate([arrays[xh], arrays[hi + xh]], 1))
            by_cos, by_sin = product[:length_y], product[length_y:]
            real = by_cos[:, :LANES] - by_sin[:, LANES:]
            imag = by_cos[:, LANES:] + by_sin[:, :LANES]
            out_ref[:, (f * 2) * hi + xh] = real.reshape(lo, cells_y, LANES)
            out_ref[:, (f * 2 + 1) * hi + xh] = imag.reshape(lo, cells_y, LANES)


def pool_matrix(rows, columns, weight, transposed):
    long_axis = 0 if transposed else 1
    shape = (columns, rows) if transposed else (rows, columns)
    long = lax.broadcasted_iota(jnp.int32, shape, long_axis)
    short = lax.broadcasted_iota(jnp.int32, shape, 1 - long_axis)
    return jnp.where(long // 2 == short, weight, 0.0).astype(jnp.float32)


def pool_rows(cells_x, cells_y):
    shape = (cells_x * cells_y // 4, cells_x * cells_y)
    short = lax.broadcasted_iota(jnp.int32, shape, 0)
    long = lax.broadcasted_iota(jnp.int32, shape, 1)
    same_x = long // (2 * cells_y) == short // (cells_y // 2)
    same_y = (long % cells_y) // 2 == short % (cells_y // 2)
    return jnp.where(same_x & same_y, 0.125, 0.0).astype(jnp.float32)


def z_back_kernel(sizes, in_ref, table_ref, modulus_ref, coarse_ref, held):
    lo, hi, kept = sizes
    cells_y = in_ref.shape[2]
    cells_x = lo * hi
    length_z = table_ref.shape[0]
    for xh in range(hi):
        tiles = {}
        for f in range(2):
            for c in range(2):
                arrays = [in_ref[p, (f * 2 + c) * hi + xh] for p in range(lo)]
                tiles[f, c] = exchange(arrays, kept)
        for xl in range(lo):
            mixed = swap_slot(tiles[0, 1][xl], tiles[1, 0][xl])
            members = ((tiles[0, 0][xl], mixed[0]), (mixed[1], tiles[1, 1][xl]))
            rows = pl.ds((xh * lo + xl) * cells_y, cells_y)
            for f in range(2):
                for c in range(2):
                    held[f, rows, pl.ds(c * LANES, LANES)] = members[f][c]
    coarse_ref[...] = jnp.zeros(coarse_ref.shape, jnp.float32)
    for f in range(2):
        values = jnp.exp(0.5 * dot(held[f], table_ref[...]))
        modulus_ref[f] = values.reshape(cells_x, cells_y, length_z)
        size_x, size_y, size_z = cells_x, cells_y, length_z
        start = 0
        for _ in range(3):
            right = pool_matrix(size_z // 2, size_z, 1.0, True)
            values = dot(pool_rows(size_x, size_y), dot(values, right))
            size_x, size_y, size_z = size_x // 2, size_y // 2, size_z // 2
            height = 2 * size_x * size_y // lo
            for d in range(lo // 2):
                piece = values[d * height : (d + 1) * height]
                place = (f * lo // 2 + d, pl.ds(start, height), pl.ds(0, size_z))
                coarse_ref[place] = piece
            start += height


def pick_kernel(heights, table_ref, in_ref, out_ref):
    for column in range(in_ref.shape[0]):
        start = 0
        for index, height in enumerate(heights):
            rows = pl.ds(start, height)
            out_ref[column, rows] = in_ref[table_ref[index, column], rows]
            start += height


def spread_kernel(axis, tail, used, in_ref, out_ref, own_sem, sends, recvs, tail_sends, tail_recvs):
    count, height = in_ref.shape[0], in_ref.shape[1]
    me = lax.axis_index(axis)
    used = used()
    rest = pl.ds(tail, height - tail)
    barrier = pltpu.get_barrier_semaphore()
    for away in range(1, count):
        peer = lax.rem(me + away, count)
        pl.semaphore_signal(barrier, inc=1, device_id={axis: peer}, device_id_type=MESH)
    own = pltpu.make_async_copy(in_ref.at[me], out_ref.at[me], own_sem)
    own.start()
    pl.semaphore_wait(barrier, count - 1)
    copies, extras = [], []
    for away in sorted(range(1, count), key=lambda a: -min(a, count - a)):
        peer = lax.rem(me + away, count)
        copy = pltpu.make_async_remote_copy(
            src_ref=in_ref.at[peer, pl.ds(0, tail)],
            dst_ref=out_ref.at[me, pl.ds(0, tail)],
            send_sem=sends.at[away],
            recv_sem=recvs.at[away],
            device_id={axis: peer},
            device_id_type=MESH,
        )
        copy.start()
        copies.append(copy)
    for source in range(1, count):
        extra = pltpu.make_async_remote_copy(
            src_ref=in_ref.at[0, rest],
            dst_ref=out_ref.at[source, rest],
            send_sem=tail_sends.at[source],
            recv_sem=tail_recvs.at[source],
            device_id={axis: 0},
            device_id_type=MESH,
        )
        pl.when((me == source) & used)(extra.start)
        extras.append(extra)
    for source in range(count):

        @pl.when((me != source) & jnp.logical_not((me == 0) & used))
        def _():
            out_ref[source, rest] = jnp.zeros(out_ref.shape[1:], jnp.float32)[tail:]

    own.wait()
    for copy in copies:
        copy.wait()
    for source in range(1, count):
        pl.when((me == source) & used)(extras[source - 1].wait_send)
        pl.when((me == 0) & used)(extras[source - 1].wait_recv)


def spread_call(values, axis, number, tail, used):
    count = values.shape[0]

    def body(*refs):
        spread_kernel(axis, tail, used, *refs)

    return pl.pallas_call(
        body,
        out_shape=jax.ShapeDtypeStruct(values.shape, values.dtype),
        in_specs=[pl.BlockSpec(memory_space=pltpu.VMEM)],
        out_specs=pl.BlockSpec(memory_space=pltpu.VMEM),
        scratch_shapes=[pltpu.SemaphoreType.DMA] + [pltpu.SemaphoreType.DMA((count,))] * 4,
        compiler_params=pltpu.CompilerParams(collective_id=number, has_side_effects=True),
    )(values)


def spread(values, axis):
    return lax.all_to_all(values, axis, split_axis=0, concat_axis=0, tiled=True)


def lanes_path(white_noise, spectrum, group_table):
    members, cells_x, cells_y, length_z = white_noise.shape
    size_px, size_py = lax.axis_size("px"), lax.axis_size("py")
    length_x, length_y = cells_x * size_px, cells_y * size_py
    lo, hi = size_py, cells_x // size_py
    kept = LANES // size_py
    sizes = (lo, hi, kept)
    f32 = jnp.float32
    params = pltpu.CompilerParams(vmem_limit_bytes=48 * 1024 * 1024)

    def call(body, shapes, *operands, scratch=(), scalars=0):
        out = [jax.ShapeDtypeStruct(shape, f32) for shape in shapes]
        specs = [pl.BlockSpec(memory_space=pltpu.SMEM)] * scalars
        specs += [pl.BlockSpec(memory_space=pltpu.VMEM)] * (len(operands) - scalars)
        return pl.pallas_call(
            body,
            out_shape=out,
            in_specs=specs,
            out_specs=[pl.BlockSpec(memory_space=pltpu.VMEM)] * len(out),
            scratch_shapes=list(scratch),
            compiler_params=params,
        )(*operands)

    z_ahead, z_back = half_tables(length_z)
    z_ahead = z_ahead.reshape(length_z, length_z)
    z_back = z_back.reshape(length_z, length_z).T * (1.0 / (length_x * length_y * length_z))
    angles = angles_of(length_y)
    y_table = jnp.asarray(np.concatenate([np.cos(angles), np.sin(angles)], 0), f32)
    lane = np.arange(LANES)
    part = (lane // (hi * size_px)) % 2
    place = (lane % size_px) * cells_x + (lane // size_px % hi) * lo + lane // kept

    def x_table(direction):
        table = complex_array(length_x, direction)
        rows = table[part, place]
        return jnp.asarray(rows[:, part, place], f32)

    first = (lax.axis_index("px") == 0) & (lax.axis_index("py") == 0)
    first = first.astype(jnp.int32).reshape(1)
    held = pltpu.VMEM((members, cells_x * cells_y, length_z), f32)

    def bind(body):
        def bound(*refs):
            body(sizes, *refs)

        return bound

    tiles = 4 * hi
    (values,) = call(
        bind(z_forward_kernel),
        [(size_py, tiles + hi + 1, cells_y, LANES)],
        white_noise,
        spectrum,
        z_ahead,
        scratch=[held],
    )
    values = spread_call(values, "py", 0, tiles + hi, lambda: True)
    (values,) = call(
        bind(y_forward_kernel), [(size_px, 3 * length_y, LANES)], values, y_table
    )
    values = spread_call(
        values, "px", 1, 2 * length_y + length_y // 2, lambda: lax.axis_index("py") == 0
    )
    (values,) = call(
        bind(x_kernel),
        [(size_px, 2 * length_y, LANES)],
        first,
        values,
        x_table(-1.0),
        x_table(1.0),
        scalars=1,
    )
    values = spread(values, "px")
    (values,) = call(
        bind(y_back_kernel), [(size_py, tiles, cells_y, LANES)], values, y_table
    )
    values = spread(values, "py")
    shapes = []
    heights = []
    size = (cells_x, cells_y, length_z)
    for _ in range(3):
        size = tuple(extent // 2 for extent in size)
        shapes.append((members,) + size)
        heights.append(members * size[0] * size[1] // size_py)
    modulus, coarse = call(
        bind(z_back_kernel),
        [white_noise.shape, (size_py, sum(heights), LANES)],
        values,
        z_back,
        scratch=[held],
    )
    coarse = spread(coarse, "py")

    def pick(*refs):
        pick_kernel(heights, *refs)

    (coarse,) = call(pick, [coarse.shape], group_table, coarse, scalars=1)
    coarse = spread(coarse, "py")
    routed, start = [], 0
    for shape, height in zip(shapes, heights):
        routed.append(coarse[:, start : start + height, : shape[3]].reshape(shape))
        start += height
    return (modulus, routed[0], routed[1], routed[2])


def on_device(white_noise, spectrum, group_table):
    members, cells_x, cells_y, length_z = white_noise.shape
    size_px, size_py = lax.axis_size("px"), lax.axis_size("py")
    fits = members == 2 and length_z == 2 * LANES and 2 * cells_x * size_px == LANES
    fits = fits and cells_x * 2 == size_px * size_py
    fits = fits and size_px * size_px * size_py == LANES
    chosen = lanes_path if fits else general_path
    return chosen(white_noise, spectrum, group_table)


def solution(mesh):
    in_specs = (P(None, "px", "py", None), P("px", "py", None), P())
    out_specs = (P(None, "px", "py", None),) * 4
    return jax.shard_map(
        on_device, mesh=mesh, in_specs=in_specs, out_specs=out_specs, check_vma=False
    )
```
